256 devices in a mesh: unit: 4 (over y), bank: 4 (over x), zero: 16 (over z, core).
Axes of the slice: x: 4, y: 4, z: 8, core: 2. Of those that a mesh axis runs over, the one named last changes fastest.
Arguments:
- train_down: float32 [256, 1024, 2048], P(('unit', 'bank'), None, 'zero'), parts along dimension 0, may hold values from -0.25 to 0.25
- router_weight: float32 [8192, 64], P(('unit', 'zero'), 'bank'), parts along dimension 0, may hold values from -0.125 to 0.125
- router_gain: float32 [8192], P(('unit', 'zero')), parts along dimension 0, may hold values from 0.25 to 1.75
Outputs:
- ready_down: bfloat16 [256, 1024, 2048], P(('unit', 'bank'), 'zero'), parts along dimension 0
- scale_down: float32 [256, 1024], P(('unit', 'bank'), 'zero'), parts along dimension 0
- serve_router: bfloat16 [8192, 64], P('unit'), parts along dimension 0
The draws below stay inside these ranges and needn't reach their ends.
There are 4 independent parts, one for each index of `unit`. The reference program is written for one: setup_inputs(seed, part) draws one part's arguments, and reference() takes and returns one part's arrays. A program takes and returns all parts, laid end to end along the dimension named above; each array names one. Nothing has to cross between parts.
All inputs are finite; a program needn't handle non-finite values.
Results may differ from the reference program's by a relative error of at most 0.001.
Values may be sent and summed in bfloat16 or wider, within the bound.
No kernel may reach another device: no remote copies, remote signals or barrier semaphores. Data moves between devices by JAX's collectives and lax.ppermute only.
A program may use at most 128 MiB of HBM per device.

```python
import jax
import jax.numpy as jnp

EXPERTS = 64
D_MODEL = 2048
D_EXPERT = 1024


def with_spikes(drawn, own_key, source, target, parts, factor):
    owner, partner = [(jnp.arange(drawn.shape[axis_at]) // (drawn.shape[axis_at] // parts)).reshape([-1 if axis == axis_at else 1 for axis in range(drawn.ndim)]) for axis_at in (source, target)]
    chosen = jax.random.permutation(own_key, parts)[partner]
    strong = (owner == chosen) | (owner == (partner + parts // 2) % parts)
    return jnp.where(strong, factor * drawn, drawn)


def levels(rng, extent, split, smallest, high):
    gain = 1.0
    for position, shards_of in split:
        draws = jax.random.uniform(jax.random.fold_in(jax.random.fold_in(rng, 6), position), (shards_of,), jnp.float32, smallest / len(split), high / len(split))
        gain = gain * jnp.repeat(jnp.exp(draws), extent[position] // shards_of).reshape((-1,) + (1,) * (len(extent) - 1 - position))
    return gain


def gaussian(own_key, dims, spread, most, shards=(), dtype=jnp.bfloat16):
    array = jax.random.normal(own_key, dims, jnp.float32) * spread
    if len(shards) > 0:
        array = levels(own_key, dims, shards, -0.22, 0.18) * array
    return jnp.clip(array, min=-most, max=most).astype(dtype)


def bell_draw_with(stream_key, extent, width, bound, pieces, heavy, held_as=jnp.bfloat16):
    entries = width * jax.random.normal(stream_key, extent, jnp.float32)
    if pieces:
        entries = entries * levels(stream_key, extent, pieces, -0.22, 0.18)
    return jnp.clip(with_spikes(entries, jax.random.fold_in(stream_key, 3), *heavy), -bound, bound).astype(held_as)


def setup_inputs(seed: int = 0, part: int = 0) -> dict:
    seeds = jax.random.split(jax.random.key(seed), 4)
    part_keys = jax.random.split(jax.random.fold_in(seeds[3], part), 4)
    return {
        "train_down": bell_draw_with(part_keys[0], (EXPERTS, D_EXPERT, D_MODEL), D_EXPERT ** -0.5, 0.25, ((0, 4), (2, 16)), (2, 1, 16, 2.0), jnp.float32),
        "router_weight": gaussian(part_keys[1], (D_MODEL, EXPERTS), D_MODEL ** -0.5, 0.125, ((0, 16), (1, 4)), jnp.float32),
        "router_gain": jnp.clip(1.0 + 0.15 * jax.random.normal(part_keys[2], (D_MODEL,), jnp.float32), 0.25, 1.75),
    }


def reference(train_down, router_weight, router_gain):
    scale_down = jnp.max(jnp.abs(train_down), axis=2)
    ready_down = (train_down / jnp.expand_dims(scale_down, 2)).astype(jnp.bfloat16)
    serve_router = (router_weight * router_gain[:, None]).astype(jnp.bfloat16)
    return ready_down, scale_down, serve_router
```

```python
import functools

import jax
import jax.numpy as jnp
from jax import lax
from jax.experimental import pallas as pl
from jax.experimental.pallas import tpu as pltpu
from jax.sharding import Mesh
from jax.sharding import PartitionSpec as P

ZERO = ("zero_0", "zero_1")
UNIT_ZERO = ("unit", "zero_0", "zero_1")

OFFSETS = ((4, 0), (3, 0), (-3, 0), (4, 1), (3, 1), (-3, 1), (2, 0), (-2, 0), (2, 1), (-2, 1), (1, 0), (-1, 0), (1, 1), (-1, 1))
GROUPS = (7, 5, 2)
VMEM = pl.BlockSpec(memory_space=pltpu.VMEM)
ANY = pl.BlockSpec(memory_space=pl.ANY)
HBM = pl.BlockSpec(memory_space=pltpu.HBM)
LIMIT = 8 * 1024 * 1024


def maxima_kernel(x_ref, out_ref, held_ref, sems):
    experts, owners = x_ref.shape[0], out_ref.shape[0]
    lane = lax.broadcasted_iota(jnp.int32, (8, 128), 1)

    def copy(e):
        return pltpu.make_async_copy(x_ref.at[e], held_ref.at[e], sems.at[e])

    for e in range(experts):
        copy(e).start()

    @pl.loop(0, experts)
    def _(e):
        copy(e).wait()
        here = [lane == e * 8 + r for r in range(8)]
        for k in range(owners):
            tile = jnp.where(e == 0, jnp.zeros((8, 128), jnp.float32), out_ref[k])
            for r in range(8):
                row = k * 64 + r * 8
                top = jnp.max(jnp.abs(held_ref[e, row : row + 8, :]), axis=1, keepdims=True)
                tile = jnp.where(here[r], top, tile)
            out_ref[k] = tile


def local_maxima(x):
    experts, rows, lanes = x.shape
    return pl.pallas_call(
        maxima_kernel,
        in_specs=[HBM],
        out_specs=VMEM,
        out_shape=jax.ShapeDtypeStruct((rows // 64, 8, 128), jnp.float32),
        scratch_shapes=[pltpu.VMEM(x.shape, jnp.float32), pltpu.SemaphoreType.DMA((experts,))],
        compiler_params=pltpu.CompilerParams(vmem_limit_bytes=7 * LIMIT),
        name="local_maxima",
    )(x)


def combine_kernel(got_ref, weight_ref, gain_ref, own_ref, out_ref):
    own = jnp.max(got_ref[...], axis=0)
    own_ref[...] = own
    router = weight_ref[...] * gain_ref[...]
    for k in range(out_ref.shape[0]):
        out_ref[k, 0:8, :] = own
        out_ref[k, 8:24, :] = router


def combined(got, weight, gain):
    return pl.pallas_call(
        combine_kernel,
        in_specs=[VMEM] * 3,
        out_specs=[VMEM] * 2,
        out_shape=[
            jax.ShapeDtypeStruct((8, 128), jnp.float32),
            jax.ShapeDtypeStruct((got.shape[0], 24, 128), jnp.float32),
        ],
        compiler_params=pltpu.CompilerParams(vmem_limit_bytes=LIMIT),
        name="combine",
    )(got, weight, gain)


def device_at(offset):
    z, c = lax.axis_index("zero_0"), lax.axis_index("zero_1")
    return lax.rem(z + offset[0] + 8, 8) * 2 + lax.rem(c + offset[1], 2)


def divide_kernel(offset, x_ref, scales_ref, out_ref, rows_ref, scale_ref, sems, scale_sem):
    k = device_at(offset)
    steps = sems.shape[0]
    experts = x_ref.shape[0]
    each = experts // steps
    first = pl.multiple_of(k * 64, 64)
    scale_copy = pltpu.make_async_copy(scales_ref.at[k, pl.ds(0, 8), :], scale_ref, scale_sem)
    scale_copy.start()
    copies = [
        pltpu.make_async_copy(
            x_ref.at[pl.ds(i * each, each), pl.ds(first, 64), :], rows_ref.at[pl.ds(i * each, each)], sems.at[i]
        )
        for i in range(steps)
    ]
    for copy in copies:
        copy.start()
    scale_copy.wait()
    scale = scale_ref[...]
    for i, copy in enumerate(copies):
        copy.wait()
        for e in range(i * each, (i + 1) * each):
            for r in range(0, 8, 2):
                halves = [
                    rows_ref[e, (r + h) * 8 : (r + h) * 8 + 8, :] / scale[:, e * 8 + r + h : e * 8 + r + h + 1]
                    for h in range(2)
                ]
                out_ref[e, r * 8 : r * 8 + 16, :] = jnp.concatenate(halves, axis=0).astype(jnp.bfloat16)


def divided(offset, x, scales):
    experts = x.shape[0]
    return pl.pallas_call(
        functools.partial(divide_kernel, offset),
        in_specs=[HBM, ANY],
        out_specs=VMEM,
        out_shape=jax.ShapeDtypeStruct((experts, 64, 128), jnp.bfloat16),
        scratch_shapes=[
            pltpu.VMEM((experts, 64, 128), jnp.float32),
            pltpu.VMEM((8, 128), jnp.float32),
            pltpu.SemaphoreType.DMA((4,)),
            pltpu.SemaphoreType.DMA,
        ],
        compiler_params=pltpu.CompilerParams(vmem_limit_bytes=LIMIT),
        cost_estimate=pl.CostEstimate(flops=experts * 64 * 128 * 8, bytes_accessed=experts * 64 * 128 * 6, transcendentals=0),
        name="divide",
    )(x, scales)


def place_kernel(offsets, *refs):
    n = len(offsets)
    pieces, out_ref, sems = refs[:n], refs[-2], refs[-1]
    copies = []
    for i, offset in enumerate(offsets):
        column = pl.multiple_of(device_at((-offset[0], offset[1])) * 128, 128)
        copies.append(pltpu.make_async_copy(pieces[i], out_ref.at[:, :, pl.ds(column, 128)], sems.at[i]))
    for copy in copies:
        copy.start()
    for copy in copies:
        copy.wait()


def placed(offsets, pieces, into):
    n = len(offsets)
    experts = pieces[0].shape[0]
    out = jax.ShapeDtypeStruct((experts, 64, 2048), jnp.bfloat16)
    return pl.pallas_call(
        functools.partial(place_kernel, tuple(offsets)),
        in_specs=[VMEM] * n + ([] if into is None else [ANY]),
        out_specs=ANY,
        out_shape=out,
        scratch_shapes=[pltpu.SemaphoreType.DMA((n,))],
        input_output_aliases={} if into is None else {n: 0},
        compiler_params=pltpu.CompilerParams(vmem_limit_bytes=LIMIT),
        cost_estimate=pl.CostEstimate(flops=n * experts * 64 * 128, bytes_accessed=n * experts * 64 * 128 * 4, transcendentals=0),
        name="place",
    )(*pieces, *([] if into is None else [into]))


def sent(piece, offset):
    pairs = [(z * 2 + c, ((z + offset[0]) % 8) * 2 + (c + offset[1]) % 2) for z in range(8) for c in range(2)]
    return lax.ppermute(piece, ZERO, pairs)


def per_device(train_down, router_weight, router_gain):
    got = lax.all_to_all(local_maxima(train_down), ZERO, 0, 0, tiled=True)
    own, payload = combined(got, router_weight.T, router_gain[None, :])
    shared = lax.all_to_all(payload, ZERO, 0, 0, tiled=True)

    pieces = [sent(divided(offset, train_down, shared), offset) for offset in OFFSETS]
    near = sent(divided((0, 1), train_down, shared), (0, 1))
    kept = divided((0, 0), train_down, shared)

    offsets = ((0, 0), (0, 1)) + OFFSETS
    pieces = [kept, near] + pieces
    ready_down, first = None, 0
    for n in GROUPS:
        last = first + n + (2 if first == 0 else 0)
        ready_down = placed(offsets[first:last], pieces[first:last], ready_down)
        first = last

    scale_down = own.reshape(8, 16, 8).transpose(1, 2, 0).reshape(16, 64)

    rows = shared[:, 8:24, :].astype(jnp.bfloat16).transpose(1, 0, 2).reshape(16, 2048)
    rows, _ = lax.optimization_barrier((rows, pieces[5]))
    serve_router = lax.all_gather(rows, "bank", axis=0, tiled=True).T
    return (ready_down, scale_down, serve_router)


def solution(mesh):
    torus = Mesh(
        mesh.devices.reshape(mesh.shape["unit"], mesh.shape["bank"], 8, 2),
        ("unit", "bank", "zero_0", "zero_1"),
    )
    placed_at = (P(("unit", "bank"), None, ZERO), P(UNIT_ZERO, "bank"), P(UNIT_ZERO))
    return jax.shard_map(
        per_device,
        mesh=torus,
        in_specs=placed_at,
        out_specs=(P(("unit", "bank"), ZERO, None), P(("unit", "bank"), ZERO), P("unit", None)),
        check_vma=False,
    )
```

```python
import functools

import jax
import jax.numpy as jnp
from jax import lax
from jax.experimental import pallas as pl
from jax.experimental.pallas import tpu as pltpu
from jax.sharding import Mesh
from jax.sharding import PartitionSpec as P


ZERO = ("zero_0", "zero_1")
UNIT_ZERO = ("unit", "zero_0", "zero_1")

RAW = (((4, 0), 0, 7), ((2, 0), 0, 6), ((-2, 0), 0, 5), ((2, 1), 0, 6), ((-2, 1), 0, 8))
FIRST = (0,)
PIECES = (
    ((3, 0), 0, 16),
    ((-3, 0), 0, 16),
    ((4, 0), 7, 9),
    ((1, 0), 0, 16),
    ((-1, 0), 0, 16),
    ((3, 1), 0, 16),
    ((-3, 1), 0, 16),
    ((4, 1), 0, 16),
    ((0, 1), 0, 16),
    ((1, 1), 0, 16),
    ((-1, 1), 0, 16),
    ((2, 0), 6, 10),
    ((-2, 0), 5, 11),
    ((2, 1), 6, 10),
    ((-2, 1), 8, 8),
)
GROUPS = (10, 6, 3, 2)
VMEM = pl.BlockSpec(memory_space=pltpu.VMEM)
ANY = pl.BlockSpec(memory_space=pl.ANY)
LIMIT = 4 * 1024 * 1024
WIDE = 50 * 1024 * 1024


def maxima_kernel(pieces, x_ref, out_ref, *refs):
    held_ref, sems, pick_sems = refs[len(pieces) :]
    experts, owners = x_ref.shape[0], out_ref.shape[0]
    lane = lax.broadcasted_iota(jnp.int32, (8, 128), 1)

    def copy(e):
        return pltpu.make_async_copy(x_ref.at[e], held_ref.at[e], sems.at[e])

    for e in range(experts):
        copy(e).start()
    picks = [pick(piece, x_ref, ref, pick_sems.at[i]) for i, (piece, ref) in enumerate(zip(pieces, refs))]
    for each in picks:
        each.start()

    @pl.loop(0, experts // 4)
    def _(g):
        for e in range(4):
            copy(g * 4 + e).wait()
        for k in range(owners):
            tile = jnp.where(g == 0, jnp.zeros((8, 128), jnp.float32), out_ref[k])
            for e in range(4):
                for r in range(8):
                    row = k * 64 + r * 8
                    top = jnp.max(jnp.abs(held_ref[g * 4 + e, row : row + 8, :]), axis=1, keepdims=True)
                    tile = jnp.where(lane == (g * 4 + e) * 8 + r, top, tile)
            out_ref[k] = tile

    for each in picks:
        each.wait()


def local_maxima(x, pieces):
    experts, rows, lanes = x.shape
    picks = [jax.ShapeDtypeStruct((piece[2], 64, lanes), jnp.float32) for piece in pieces]
    return pl.pallas_call(
        functools.partial(maxima_kernel, pieces),
        in_specs=[ANY],
        out_specs=[VMEM] * (1 + len(picks)),
        out_shape=[jax.ShapeDtypeStruct((rows // 64, 8, 128), jnp.float32)] + picks,
        scratch_shapes=[
            pltpu.VMEM(x.shape, jnp.float32),
            pltpu.SemaphoreType.DMA((experts,)),
            pltpu.SemaphoreType.DMA((len(picks),)),
        ],
        compiler_params=pltpu.CompilerParams(vmem_limit_bytes=WIDE),
        name="local_maxima",
    )(x)


def combine_kernel(got_ref, weight_ref, gain_ref, own_ref, out_ref):
    own = jnp.max(got_ref[...], axis=0)
    own_ref[...] = own
    router = weight_ref[...] * gain_ref[...]
    for k in range(out_ref.shape[0]):
        out_ref[k, 0:8, :] = own
        out_ref[k, 8:24, :] = router


def combined(got, weight, gain):
    return pl.pallas_call(
        combine_kernel,
        in_specs=[VMEM] * 3,
        out_specs=[VMEM] * 2,
        out_shape=[
            jax.ShapeDtypeStruct((8, 128), jnp.float32),
            jax.ShapeDtypeStruct((got.shape[0], 24, 128), jnp.float32),
        ],
        compiler_params=pltpu.CompilerParams(vmem_limit_bytes=LIMIT),
        name="combine",
    )(got, weight, gain)


def device_at(offset):
    z, c = lax.axis_index("zero_0"), lax.axis_index("zero_1")
    return lax.rem(z + offset[0] + 8, 8) * 2 + lax.rem(c + offset[1], 2)


def pick(piece, x_ref, out_ref, sem):
    offset, start, count = piece
    first = pl.multiple_of(device_at(offset) * 64, 64)
    return pltpu.make_async_copy(x_ref.at[pl.ds(start, count), pl.ds(first, 64), :], out_ref, sem)


def pick_kernel(piece, x_ref, out_ref, sem):
    copy = pick(piece, x_ref, out_ref, sem)
    copy.start()
    copy.wait()


def picked(piece, x):
    return pl.pallas_call(
        functools.partial(pick_kernel, piece),
        in_specs=[ANY],
        out_specs=VMEM,
        out_shape=jax.ShapeDtypeStruct((piece[2], 64, 128), jnp.float32),
        scratch_shapes=[pltpu.SemaphoreType.DMA],
        compiler_params=pltpu.CompilerParams(vmem_limit_bytes=WIDE),
        cost_estimate=pl.CostEstimate(flops=2000000, bytes_accessed=piece[2] * 64 * 128 * 8, transcendentals=0),
        name="pick",
    )(x)


def divide_rows(rows_ref, out_ref, scale, experts, start):
    for e in experts:
        for r in range(0, 8, 2):
            lane = (start + e) * 8 + r
            both = jnp.concatenate([scale[:, lane : lane + 1], scale[:, lane + 1 : lane + 2]], axis=0)
            out_ref[e, r * 8 : r * 8 + 16, :] = (rows_ref[e, r * 8 : r * 8 + 16, :] / both).astype(jnp.bfloat16)


def divide_kernel(piece, x_ref, scales_ref, out_ref, rows_ref, sems):
    offset, start, count = piece
    k = device_at(offset)
    first = pl.multiple_of(k * 64, 64)
    parts = [range(e, min(e + 4, count)) for e in range(0, count, 4)]
    copies = [
        pltpu.make_async_copy(
            x_ref.at[pl.ds(start + part[0], len(part)), pl.ds(first, 64), :],
            rows_ref.at[pl.ds(part[0], len(part))],
            sems.at[i],
        )
        for i, part in enumerate(parts)
    ]
    for copy in copies:
        copy.start()
    scale = scales_ref[k, 0:8, :]
    for copy, part in zip(copies, parts):
        copy.wait()
        divide_rows(rows_ref, out_ref, scale, part, start)


def divided(piece, x, scales):
    count = piece[2]
    return pl.pallas_call(
        functools.partial(divide_kernel, piece),
        in_specs=[ANY, VMEM],
        out_specs=VMEM,
        out_shape=jax.ShapeDtypeStruct((count, 64, 128), jnp.bfloat16),
        scratch_shapes=[pltpu.VMEM((count, 64, 128), jnp.float32), pltpu.SemaphoreType.DMA((pl.cdiv(count, 4),))],
        compiler_params=pltpu.CompilerParams(vmem_limit_bytes=WIDE),
        cost_estimate=pl.CostEstimate(flops=count * 64 * 128 * 8, bytes_accessed=count * 64 * 128 * 6, transcendentals=0),
        name="divide",
    )(x, scales)


def finish_kernel(piece, rows_ref, own_ref, out_ref):
    divide_rows(rows_ref, out_ref, own_ref[...], range(piece[2]), piece[1])


def finished(piece, rows, own):
    count = piece[2]
    return pl.pallas_call(
        functools.partial(finish_kernel, piece),
        in_specs=[VMEM, VMEM],
        out_specs=VMEM,
        out_shape=jax.ShapeDtypeStruct((count, 64, 128), jnp.bfloat16),
        compiler_params=pltpu.CompilerParams(vmem_limit_bytes=LIMIT),
        cost_estimate=pl.CostEstimate(flops=count * 64 * 128 * 8, bytes_accessed=count * 64 * 128 * 6, transcendentals=0),
        name="finish",
    )(rows, own)


def place_kernel(pieces, held, routed, *refs):
    n = len(pieces)
    blocks, refs = refs[:n], refs[n + held :]
    out_ref, sems = refs[routed], refs[-1]
    copies = []
    for i, (offset, start, count) in enumerate(pieces):
        column = pl.multiple_of(device_at((-offset[0], offset[1])) * 128, 128)
        target = out_ref.at[pl.ds(start, count), :, pl.ds(column, 128)]
        copies.append(pltpu.make_async_copy(blocks[i], target, sems.at[i]))
    if routed:
        copies.append(pltpu.make_async_copy(refs[0], refs[2], sems.at[n]))
    for copy in copies:
        copy.start()
    for copy in copies:
        copy.wait()


def placed(pieces, blocks, shape, into=None, router=None):
    n, held, routed = len(pieces), int(into is not None), int(router is not None)
    size = sum(piece[2] for piece in pieces) * 64 * 128
    shapes = [jax.ShapeDtypeStruct(shape, jnp.bfloat16)]
    if routed:
        shapes.append(jax.ShapeDtypeStruct(router.shape, router.dtype))
    return pl.pallas_call(
        functools.partial(place_kernel, tuple(pieces), held, routed),
        in_specs=[VMEM] * n + [ANY] * held + [VMEM] * routed,
        out_specs=[ANY] * (1 + routed),
        out_shape=shapes,
        scratch_shapes=[pltpu.SemaphoreType.DMA((n + routed,))],
        input_output_aliases={n: 0} if held else {},
        compiler_params=pltpu.CompilerParams(vmem_limit_bytes=LIMIT),
        cost_estimate=pl.CostEstimate(flops=size, bytes_accessed=size * 4, transcendentals=0),
        name="place",
    )(*blocks, *([into] if held else []), *([router] if routed else []))


def sent(piece, offset):
    pairs = [(z * 2 + c, ((z + offset[0]) % 8) * 2 + (c + offset[1]) % 2) for z in range(8) for c in range(2)]
    return lax.ppermute(piece, ZERO, pairs)


def exchanged(value):
    return lax.all_to_all(value, ZERO, 0, 0, tiled=True)


def sent_raw(i, rows):
    return sent(rows, RAW[i][0])


def per_device(train_down, router_weight, router_gain):
    experts = train_down.shape[0]
    rows = [picked(RAW[i], train_down) for i in FIRST]
    maxima, *more = local_maxima(train_down, RAW[len(FIRST) :])
    raw = [sent_raw(i, r) for i, r in enumerate(rows + more)]
    got = exchanged(maxima)
    own, payload = combined(got, router_weight.T, router_gain[None, :])
    shared = exchanged(payload)

    kept = ((0, 0), 0, experts)
    blocks = []
    for piece in PIECES:
        blocks.append(sent(divided(piece, train_down, shared), piece[0]))

    rows = shared[:, 8:24, :].astype(jnp.bfloat16).transpose(1, 0, 2).reshape(16, 2048)
    rows, _ = lax.optimization_barrier((rows, blocks[2]))
    router = lax.all_gather(rows, "bank", axis=0, tiled=True)

    early = [divided(kept, train_down, shared)] + [finished(p, r, own) for p, r in zip(RAW, raw)]
    pieces, blocks = (kept,) + RAW + PIECES, early + blocks
    shape = (experts, 64, 2048)
    ready_down, first = None, 0
    for i, n in enumerate(GROUPS):
        group = slice(first, first + n)
        out = placed(pieces[group], blocks[group], shape, ready_down, router if i == 1 else None)
        ready_down, first = out[0], first + n
        if i == 1:
            serve_router = out[1].T

    scale_down = own.reshape(8, 16, 8).transpose(1, 2, 0).reshape(16, 64)
    return (ready_down, scale_down, serve_router)


def solution(mesh):
    torus = Mesh(
        mesh.devices.reshape(mesh.shape["unit"], mesh.shape["bank"], 8, 2),
        ("unit", "bank", "zero_0", "zero_1"),
    )
    placed_at = (P(("unit", "bank"), None, ZERO), P(UNIT_ZERO, "bank"), P(UNIT_ZERO))
    return jax.shard_map(
        per_device,
        mesh=torus,
        in_specs=placed_at,
        out_specs=(P(("unit", "bank"), ZERO, None), P(("unit", "bank"), ZERO), P("unit", None)),
        check_vma=False,
    )
```

```python
import functools

import jax
import jax.numpy as jnp
from jax import lax
from jax.experimental import pallas as pl
from jax.experimental.pallas import tpu as pltpu
from jax.sharding import Mesh
from jax.sharding import PartitionSpec as P


ZERO = ("zero_0", "zero_1")
UNIT_ZERO = ("unit", "zero_0", "zero_1")

OWN, OTHER = -1, -2
RAW = (((4, 0), 0, 8), ((2, 0), 0, 5), ((-2, 0), 0, 7))
PIECES = (
    ((3, 0), OWN, 8),
    ((-3, 0), OWN, 8),
    ((4, 0), 8, 8),
    ((3, 1), 0, 16),
    ((-3, 1), 0, 16),
    ((1, 0), 0, 16),
    ((-1, 0), 0, 16),
    ((4, 1), 0, 16),
    ((3, 0), OTHER, 8),
    ((-3, 0), OTHER, 8),
    ((0, 1), 0, 16),
    ((1, 1), 0, 16),
    ((-1, 1), 0, 16),
    ((2, 0), 5, 11),
    ((-2, 0), 7, 9),
    ((2, 1), 0, 16),
    ((-2, 1), 0, 16),
)
READY = 2
GROUPS = (10, 6, 3, 2)
VMEM = pl.BlockSpec(memory_space=pltpu.VMEM)
ANY = pl.BlockSpec(memory_space=pl.ANY)
LIMIT = 4 * 1024 * 1024
WIDE = 50 * 1024 * 1024
HALF = (8, 8, 128)


def f32(*shape):
    return jax.ShapeDtypeStruct(shape, jnp.float32)


def bf16(*shape):
    return jax.ShapeDtypeStruct(shape, jnp.bfloat16)


def cost(elements, bytes_each):
    return pl.CostEstimate(flops=elements * 8, bytes_accessed=elements * bytes_each, transcendentals=0)


def there(offset):
    z, c = lax.axis_index("zero_0"), lax.axis_index("zero_1")
    return lax.rem(z + offset[0] + 8, 8), lax.rem(c + offset[1], 2)


def expert_of(start, core):
    return start if start >= 0 else core * 8 if start == OWN else (1 - core) * 8


def pick(piece, x_ref, out_ref, sem):
    offset, start, count = piece
    z, c = there(offset)
    first = pl.multiple_of((z * 2 + c) * 64, 64)
    expert = expert_of(start, lax.axis_index("zero_1"))
    return pltpu.make_async_copy(x_ref.at[pl.ds(expert, count), pl.ds(first, 64), :], out_ref, sem)


def pick_kernel(pieces, x_ref, *refs):
    copies = [pick(piece, x_ref, ref, refs[-1].at[i]) for i, (piece, ref) in enumerate(zip(pieces, refs))]
    for copy in copies:
        copy.start()
    for copy in copies:
        copy.wait()


def picked(pieces, x):
    return pl.pallas_call(
        functools.partial(pick_kernel, pieces),
        in_specs=[ANY],
        out_specs=[VMEM] * len(pieces),
        out_shape=[f32(piece[2], 64, 128) for piece in pieces],
        scratch_shapes=[pltpu.SemaphoreType.DMA((len(pieces),))],
        compiler_params=pltpu.CompilerParams(vmem_limit_bytes=WIDE),
        cost_estimate=cost(sum(piece[2] for piece in pieces) * 64 * 128, 8),
        name="pick",
    )(x)


def maxima_kernel(pieces, x_ref, keep_ref, give_ref, *refs):
    halves_ref, held_ref, sems, pick_sems = refs[len(pieces) :]
    experts = x_ref.shape[0]
    lane = lax.broadcasted_iota(jnp.int32, (8, 128), 1)

    def copy(e):
        return pltpu.make_async_copy(x_ref.at[e], held_ref.at[e], sems.at[e])

    for e in range(experts):
        copy(e).start()
    picks = [pick(piece, x_ref, ref, pick_sems.at[i]) for i, (piece, ref) in enumerate(zip(pieces, refs))]
    for each in picks:
        each.start()

    @pl.loop(0, experts // 4)
    def _(g):
        half, part = g // 2, lax.rem(g, 2)
        for e in range(4):
            copy(g * 4 + e).wait()
        for q in range(8):
            tile = jnp.where(part == 0, jnp.zeros((8, 128), jnp.float32), halves_ref[half, q])
            for j in range(2):
                for e in range(4):
                    for r in range(8):
                        row = (q * 2 + j) * 64 + r * 8
                        top = jnp.max(jnp.abs(held_ref[g * 4 + e, row : row + 8, :]), axis=1, keepdims=True)
                        tile = jnp.where(lane == j * 64 + (part * 4 + e) * 8 + r, top, tile)
            halves_ref[half, q] = tile

    low = lax.axis_index("zero_1") == 0
    keep_ref[...] = jnp.where(low, halves_ref[0], halves_ref[1])
    give_ref[...] = jnp.where(low, halves_ref[1], halves_ref[0])
    for each in picks:
        each.wait()


def local_maxima(x, pieces):
    return pl.pallas_call(
        functools.partial(maxima_kernel, pieces),
        in_specs=[ANY],
        out_specs=[VMEM] * (2 + len(pieces)),
        out_shape=[f32(*HALF), f32(*HALF)] + [f32(piece[2], 64, 128) for piece in pieces],
        scratch_shapes=[
            pltpu.VMEM((2, *HALF), jnp.float32),
            pltpu.VMEM(x.shape, jnp.float32),
            pltpu.SemaphoreType.DMA((x.shape[0],)),
            pltpu.SemaphoreType.DMA((len(pieces),)),
        ],
        compiler_params=pltpu.CompilerParams(vmem_limit_bytes=WIDE),
        name="local_maxima",
    )(x)


def chip_kernel(keep_ref, got_ref, weight_ref, gain_ref, out_ref):
    both = jnp.maximum(keep_ref[...], got_ref[...])
    router = weight_ref[...] * gain_ref[...]
    for q in range(8):
        out_ref[q, 0:8] = both
        out_ref[q, 8] = router[0:8]
        out_ref[q, 9] = router[8:16]


def chip_maxima(keep, got, weight, gain):
    return pl.pallas_call(
        chip_kernel,
        in_specs=[VMEM] * 4,
        out_specs=VMEM,
        out_shape=f32(8, 10, 8, 128),
        compiler_params=pltpu.CompilerParams(vmem_limit_bytes=LIMIT),
        name="chip",
    )(keep, got, weight, gain)


def joint_kernel(shared_ref, mine_ref, router_ref):
    top = shared_ref[0, 0:8]
    for q in range(1, 8):
        top = jnp.maximum(top, shared_ref[q, 0:8])
    mine_ref[...] = top
    for q in range(8):
        router_ref[q] = jnp.concatenate([shared_ref[q, 8], shared_ref[q, 9]], axis=0).astype(jnp.bfloat16)


def joined(shared):
    return pl.pallas_call(
        joint_kernel,
        in_specs=[VMEM],
        out_specs=[VMEM] * 2,
        out_shape=[f32(*HALF), bf16(8, 16, 128)],
        compiler_params=pltpu.CompilerParams(vmem_limit_bytes=LIMIT),
        name="joint",
    )(shared)


def route_kernel(mine_ref, their_ref, out_ref):
    low = lax.axis_index("zero_1") == 0
    for q in range(8):
        mine, theirs = mine_ref[q], their_ref[q]
        out_ref[:, q * 256 : q * 256 + 128] = jnp.where(low, mine, theirs)
        out_ref[:, q * 256 + 128 : q * 256 + 256] = jnp.where(low, theirs, mine)


def routed(mine, theirs):
    return pl.pallas_call(
        route_kernel,
        in_specs=[VMEM] * 2,
        out_specs=VMEM,
        out_shape=bf16(16, 2048),
        compiler_params=pltpu.CompilerParams(vmem_limit_bytes=LIMIT),
        name="route",
    )(mine, theirs)


def scales_at(refs, offset):
    z, c = there(offset)
    tiles = [ref[z] for ref in refs]
    return [jnp.where(c == 0, tile[:, 0:64], tile[:, 64:128]) for tile in tiles]


def scales_in_order(refs, offset):
    own, other = scales_at(refs, offset)
    low = lax.axis_index("zero_1") == 0
    return [jnp.where(low, own, other), jnp.where(low, other, own)]


def divide_rows(rows_ref, out_ref, scales, experts, start):
    for e in experts:
        scale = scales[(start + e) // 8]
        for r in range(0, 8, 2):
            lane = (start + e) % 8 * 8 + r
            both = jnp.concatenate([scale[:, lane : lane + 1], scale[:, lane + 1 : lane + 2]], axis=0)
            out_ref[e, r * 8 : r * 8 + 16, :] = (rows_ref[e, r * 8 : r * 8 + 16, :] / both).astype(jnp.bfloat16)


def ready_kernel(offset, rows_ref, mine_ref, out_ref):
    divide_rows(rows_ref, out_ref, scales_at([mine_ref], offset), range(8), 0)


def ready(piece, rows, mine):
    return pl.pallas_call(
        functools.partial(ready_kernel, piece[0]),
        in_specs=[VMEM, VMEM],
        out_specs=VMEM,
        out_shape=bf16(8, 64, 128),
        compiler_params=pltpu.CompilerParams(vmem_limit_bytes=LIMIT),
        cost_estimate=cost(8 * 64 * 128, 6),
        name="ready",
    )(rows, mine)


def divide_kernel(piece, x_ref, mine_ref, their_ref, out_ref, rows_ref, sems):
    offset, start, count = piece
    z, c = there(offset)
    first = pl.multiple_of((z * 2 + c) * 64, 64)
    expert = expert_of(start, lax.axis_index("zero_1"))
    parts = [range(e, min(e + 4, count)) for e in range(0, count, 4)]
    copies = [
        pltpu.make_async_copy(
            x_ref.at[pl.ds(expert + part[0], len(part)), pl.ds(first, 64), :],
            rows_ref.at[pl.ds(part[0], len(part))],
            sems.at[i],
        )
        for i, part in enumerate(parts)
    ]
    for copy in copies:
        copy.start()
    if start == OTHER:
        scales, start = scales_at([their_ref], offset), 0
    else:
        scales = scales_in_order([mine_ref, their_ref], offset)
    for copy, part in zip(copies, parts):
        copy.wait()
        divide_rows(rows_ref, out_ref, scales, part, start)


def divided(piece, x, mine, theirs):
    count = piece[2]
    return pl.pallas_call(
        functools.partial(divide_kernel, piece),
        in_specs=[ANY, VMEM, VMEM],
        out_specs=VMEM,
        out_shape=bf16(count, 64, 128),
        scratch_shapes=[pltpu.VMEM((count, 64, 128), jnp.float32), pltpu.SemaphoreType.DMA((pl.cdiv(count, 4),))],
        compiler_params=pltpu.CompilerParams(vmem_limit_bytes=WIDE),
        cost_estimate=cost(count * 64 * 128, 6),
        name="divide",
    )(x, mine, theirs)


def finish_kernel(pieces, *refs):
    n = len(pieces)
    rows, (mine_ref, their_ref), outs, (scale_ref, turned_ref) = refs[:n], refs[n : n + 2], refs[n + 2 : -2], refs[-2:]
    scales = scales_in_order([mine_ref, their_ref], (0, 0))
    for i, (_, start, count) in enumerate(pieces):
        divide_rows(rows[i], outs[i], scales, range(count), start)
    tile = jnp.concatenate(scales, axis=1)
    turned_ref[...] = jnp.concatenate([tile, jnp.zeros((120, 128), jnp.float32)], axis=0).T
    lane = lax.broadcasted_iota(jnp.int32, (16, 128), 1)
    out = turned_ref[pl.ds(0, 16, stride=8), :]
    for r in range(1, 8):
        part = pltpu.roll(turned_ref[pl.ds(r, 16, stride=8), :], r * 8, axis=1)
        out = jnp.where(lane >= r * 8, part, out)
    scale_ref[...] = out[:, 0:64]


def finished(pieces, rows, mine, theirs):
    n = len(pieces)
    return pl.pallas_call(
        functools.partial(finish_kernel, pieces),
        in_specs=[VMEM] * (n + 2),
        out_specs=[VMEM] * (n + 1),
        out_shape=[bf16(piece[2], 64, 128) for piece in pieces] + [f32(16, 64)],
        scratch_shapes=[pltpu.VMEM((128, 128), jnp.float32)],
        compiler_params=pltpu.CompilerParams(vmem_limit_bytes=LIMIT),
        cost_estimate=cost(sum(piece[2] for piece in pieces) * 64 * 128, 6),
        name="finish",
    )(*rows, mine, theirs)


def place_kernel(pieces, held, routed, *refs):
    n = len(pieces)
    blocks, refs = refs[:n], refs[n + held :]
    out_ref, sems = refs[routed], refs[-1]
    copies = []
    for i, (offset, start, count) in enumerate(pieces):
        z, c = there((-offset[0], offset[1]))
        column = pl.multiple_of((z * 2 + c) * 128, 128)
        target = out_ref.at[pl.ds(expert_of(start, c), count), :, pl.ds(column, 128)]
        copies.append(pltpu.make_async_copy(blocks[i], target, sems.at[i]))
    if routed:
        copies.append(pltpu.make_async_copy(refs[0], refs[2], sems.at[n]))
    for copy in copies:
        copy.start()
    for copy in copies:
        copy.wait()


def placed(pieces, blocks, shape, into=None, router=None):
    n, held, routed = len(pieces), int(into is not None), int(router is not None)
    return pl.pallas_call(
        functools.partial(place_kernel, tuple(pieces), held, routed),
        in_specs=[VMEM] * n + [ANY] * held + [VMEM] * routed,
        out_specs=[ANY] * (1 + routed),
        out_shape=[bf16(*shape)] + ([bf16(*router.shape)] if routed else []),
        scratch_shapes=[pltpu.SemaphoreType.DMA((n + routed,))],
        input_output_aliases={n: 0} if held else {},
        compiler_params=pltpu.CompilerParams(vmem_limit_bytes=LIMIT),
        cost_estimate=cost(sum(piece[2] for piece in pieces) * 64 * 128, 4),
        name="place",
    )(*blocks, *([into] if held else []), *([router] if routed else []))


def sent(piece, offset):
    pairs = [(z * 2 + c, ((z + offset[0]) % 8) * 2 + (c + offset[1]) % 2) for z in range(8) for c in range(2)]
    return lax.ppermute(piece, ZERO, pairs)


def swapped(value):
    return sent(value, (0, 1))


def per_device(train_down, router_weight, router_gain):
    experts = train_down.shape[0]
    rows = picked(RAW[:1], train_down)
    keep, give, *more = local_maxima(train_down, RAW[1:])
    raw = []
    for i, part in enumerate([*rows, *more]):
        raw.append(sent(part, RAW[i][0]))
    given = swapped(give)
    payload = chip_maxima(keep, given, router_weight.T, router_gain[None, :])
    shared = lax.all_to_all(payload, "zero_0", 0, 0, tiled=True)
    waiting = picked(PIECES[:READY], train_down)
    mine, lines = joined(shared)
    theirs = swapped(mine)

    kept = ((0, 0), 0, experts)
    blocks = []
    for i, piece in enumerate(PIECES):
        part = ready(piece, waiting[i], mine) if i < READY else divided(piece, train_down, mine, theirs)
        blocks.append(sent(part, piece[0]))

    lines = routed(lines, swapped(lines))
    lines, _ = lax.optimization_barrier((lines, blocks[2]))
    router = lax.all_gather(lines, "bank", axis=0, tiled=True)

    early = [divided(kept, train_down, mine, theirs)]
    *more, scale_down = finished(RAW, raw, mine, theirs)
    pieces, blocks = (kept,) + RAW + PIECES, [*early, *more, *blocks]
    shape = (experts, 64, 2048)
    ready_down, first = None, 0
    for i, n in enumerate(GROUPS):
        group = slice(first, first + n)
        out = placed(pieces[group], blocks[group], shape, ready_down, router if i == 1 else None)
        ready_down, first = out[0], first + n
        if i == 1:
            serve_router = out[1].T

    return (ready_down, scale_down, serve_router)


def solution(mesh):
    torus = Mesh(
        mesh.devices.reshape(mesh.shape["unit"], mesh.shape["bank"], 8, 2),
        ("unit", "bank", "zero_0", "zero_1"),
    )
    placed_at = (P(("unit", "bank"), None, ZERO), P(UNIT_ZERO, "bank"), P(UNIT_ZERO))
    return jax.shard_map(
        per_device,
        mesh=torus,
        in_specs=placed_at,
        out_specs=(P(("unit", "bank"), ZERO, None), P(("unit", "bank"), ZERO), P("unit", None)),
        check_vma=False,
    )
```

```python
import functools

import jax
import jax.numpy as jnp
from jax import lax
from jax.experimental import pallas as pl
from jax.experimental.pallas import tpu as pltpu
from jax.sharding import Mesh
from jax.sharding import PartitionSpec as P


ZERO = ("zero_0", "zero_1")
UNIT_ZERO = ("unit", "zero_0", "zero_1")

OWN, OTHER = -1, -2
RAW = (((4, 0), 0, 8), ((2, 0), 0, 10))
EARLY = 1
PIECES = (
    ((3, 0), OWN, 8),
    ((-3, 0), OWN, 8),
    ((4, 0), 8, 8),
    ((3, 1), 0, 16),
    ((-3, 1), 0, 16),
    ((1, 0), 0, 16),
    ((-1, 0), 0, 16),
    ((4, 1), 0, 16),
    ((3, 0), OTHER, 8),
    ((-3, 0), OTHER, 8),
    ((0, 1), 0, 16),
    ((2, 0), 10, 6),
    ((-2, 0), 0, 16),
    ((1, 1), 0, 16),
    ((-1, 1), 0, 16),
    ((2, 1), 0, 16),
    ((-2, 1), 0, 16),
)
READY = 2
GROUPS = (9, 6, 3, 2)
VMEM = pl.BlockSpec(memory_space=pltpu.VMEM)
ANY = pl.BlockSpec(memory_space=pl.ANY)
LIMIT = 4 * 1024 * 1024
WIDE = 50 * 1024 * 1024
HALF = (8, 8, 128)


def f32(*shape):
    return jax.ShapeDtypeStruct(shape, jnp.float32)


def bf16(*shape):
    return jax.ShapeDtypeStruct(shape, jnp.bfloat16)


def cost(elements, bytes_each):
    return pl.CostEstimate(flops=elements * 8, bytes_accessed=elements * bytes_each, transcendentals=0)


def way(core):
    return 1 - 2 * core


def there(offset):
    z, c = lax.axis_index("zero_0"), lax.axis_index("zero_1")
    return lax.rem(z + way(c) * offset[0] + 8, 8), lax.rem(c + offset[1], 2)


def sender(offset):
    c = lax.rem(lax.axis_index("zero_1") + offset[1], 2)
    return lax.rem(lax.axis_index("zero_0") - way(c) * offset[0] + 8, 8), c


def expert_of(start, core):
    return start if start >= 0 else core * 8 if start == OWN else (1 - core) * 8


def pick(piece, x_ref, out_ref, sem):
    offset, start, count = piece
    z, c = there(offset)
    first = pl.multiple_of((z * 2 + c) * 64, 64)
    expert = expert_of(start, lax.axis_index("zero_1"))
    return pltpu.make_async_copy(x_ref.at[pl.ds(expert, count), pl.ds(first, 64), :], out_ref, sem)


def pick_kernel(pieces, x_ref, *refs):
    copies = [pick(piece, x_ref, ref, refs[-1].at[i]) for i, (piece, ref) in enumerate(zip(pieces, refs))]
    for copy in copies:
        copy.start()
    for copy in copies:
        copy.wait()


def picked(pieces, x):
    return pl.pallas_call(
        functools.partial(pick_kernel, pieces),
        in_specs=[ANY],
        out_specs=[VMEM] * len(pieces),
        out_shape=[f32(piece[2], 64, 128) for piece in pieces],
        scratch_shapes=[pltpu.SemaphoreType.DMA((len(pieces),))],
        compiler_params=pltpu.CompilerParams(vmem_limit_bytes=WIDE),
        cost_estimate=cost(sum(piece[2] for piece in pieces) * 64 * 128, 8),
        name="pick",
    )(x)


def maxima_kernel(pieces, x_ref, keep_ref, give_ref, *refs):
    halves_ref, held_ref, sems, pick_sems = refs[len(pieces) :]
    experts = x_ref.shape[0]
    lane = lax.broadcasted_iota(jnp.int32, (8, 128), 1)

    def copy(e):
        return pltpu.make_async_copy(x_ref.at[e], held_ref.at[e], sems.at[e])

    for e in range(experts):
        copy(e).start()
    picks = [pick(piece, x_ref, ref, pick_sems.at[i]) for i, (piece, ref) in enumerate(zip(pieces, refs))]
    for each in picks:
        each.start()

    @pl.loop(0, experts // 4)
    def _(g):
        half, part = g // 2, lax.rem(g, 2)
        for e in range(4):
            copy(g * 4 + e).wait()
        for q in range(8):
            tile = jnp.where(part == 0, jnp.zeros((8, 128), jnp.float32), halves_ref[half, q])
            for j in range(2):
                for e in range(4):
                    for r in range(8):
                        row = (q * 2 + j) * 64 + r * 8
                        top = jnp.max(jnp.abs(held_ref[g * 4 + e, row : row + 8, :]), axis=1, keepdims=True)
                        tile = jnp.where(lane == j * 64 + (part * 4 + e) * 8 + r, top, tile)
            halves_ref[half, q] = tile

    low = lax.axis_index("zero_1") == 0
    keep_ref[...] = jnp.where(low, halves_ref[0], halves_ref[1])
    give_ref[...] = jnp.where(low, halves_ref[1], halves_ref[0])
    for each in picks:
        each.wait()


def local_maxima(x, pieces):
    return pl.pallas_call(
        functools.partial(maxima_kernel, pieces),
        in_specs=[ANY],
        out_specs=[VMEM] * (2 + len(pieces)),
        out_shape=[f32(*HALF), f32(*HALF)] + [f32(piece[2], 64, 128) for piece in pieces],
        scratch_shapes=[
            pltpu.VMEM((2, *HALF), jnp.float32),
            pltpu.VMEM(x.shape, jnp.float32),
            pltpu.SemaphoreType.DMA((x.shape[0],)),
            pltpu.SemaphoreType.DMA((len(pieces),)),
        ],
        compiler_params=pltpu.CompilerParams(vmem_limit_bytes=WIDE),
        name="local_maxima",
    )(x)


def chip_kernel(keep_ref, got_ref, weight_ref, gain_ref, out_ref):
    both = jnp.maximum(keep_ref[...], got_ref[...])
    router = weight_ref[...] * gain_ref[...]
    for q in range(8):
        out_ref[q, 0:8] = both
        out_ref[q, 8] = router[0:8]
        out_ref[q, 9] = router[8:16]


def chip_maxima(keep, got, weight, gain):
    return pl.pallas_call(
        chip_kernel,
        in_specs=[VMEM] * 4,
        out_specs=VMEM,
        out_shape=f32(8, 10, 8, 128),
        compiler_params=pltpu.CompilerParams(vmem_limit_bytes=LIMIT),
        name="chip",
    )(keep, got, weight, gain)


def joint_kernel(shared_ref, mine_ref, router_ref):
    top = shared_ref[0, 0:8]
    for q in range(1, 8):
        top = jnp.maximum(top, shared_ref[q, 0:8])
    mine_ref[...] = top
    for q in range(8):
        router_ref[q] = jnp.concatenate([shared_ref[q, 8], shared_ref[q, 9]], axis=0).astype(jnp.bfloat16)


def joined(shared):
    return pl.pallas_call(
        joint_kernel,
        in_specs=[VMEM],
        out_specs=[VMEM] * 2,
        out_shape=[f32(*HALF), bf16(8, 16, 128)],
        compiler_params=pltpu.CompilerParams(vmem_limit_bytes=LIMIT),
        name="joint",
    )(shared)


def route_kernel(mine_ref, their_ref, out_ref):
    low = lax.axis_index("zero_1") == 0
    for q in range(8):
        mine, theirs = mine_ref[q], their_ref[q]
        out_ref[:, q * 256 : q * 256 + 128] = jnp.where(low, mine, theirs)
        out_ref[:, q * 256 + 128 : q * 256 + 256] = jnp.where(low, theirs, mine)


def routed(mine, theirs):
    return pl.pallas_call(
        route_kernel,
        in_specs=[VMEM] * 2,
        out_specs=VMEM,
        out_shape=bf16(16, 2048),
        compiler_params=pltpu.CompilerParams(vmem_limit_bytes=LIMIT),
        name="route",
    )(mine, theirs)


def scales_at(refs, offset):
    z, c = there(offset)
    tiles = [ref[z] for ref in refs]
    return [jnp.where(c == 0, tile[:, 0:64], tile[:, 64:128]) for tile in tiles]


def scales_in_order(refs, offset):
    own, other = scales_at(refs, offset)
    low = lax.axis_index("zero_1") == 0
    return [jnp.where(low, own, other), jnp.where(low, other, own)]


def divide_rows(rows_ref, out_ref, scales, experts, start):
    for e in experts:
        scale = scales[(start + e) // 8]
        for r in range(0, 8, 2):
            lane = (start + e) % 8 * 8 + r
            both = jnp.concatenate([scale[:, lane : lane + 1], scale[:, lane + 1 : lane + 2]], axis=0)
            out_ref[e, r * 8 : r * 8 + 16, :] = (rows_ref[e, r * 8 : r * 8 + 16, :] / both).astype(jnp.bfloat16)


def ready_kernel(offset, rows_ref, mine_ref, out_ref):
    divide_rows(rows_ref, out_ref, scales_at([mine_ref], offset), range(8), 0)


def ready(piece, rows, mine):
    return pl.pallas_call(
        functools.partial(ready_kernel, piece[0]),
        in_specs=[VMEM, VMEM],
        out_specs=VMEM,
        out_shape=bf16(8, 64, 128),
        compiler_params=pltpu.CompilerParams(vmem_limit_bytes=LIMIT),
        cost_estimate=cost(8 * 64 * 128, 6),
        name="ready",
    )(rows, mine)


def divide_kernel(piece, x_ref, mine_ref, their_ref, out_ref, rows_ref, sems):
    offset, start, count = piece
    z, c = there(offset)
    first = pl.multiple_of((z * 2 + c) * 64, 64)
    expert = expert_of(start, lax.axis_index("zero_1"))
    parts = [range(e, min(e + 4, count)) for e in range(0, count, 4)]
    copies = [
        pltpu.make_async_copy(
            x_ref.at[pl.ds(expert + part[0], len(part)), pl.ds(first, 64), :],
            rows_ref.at[pl.ds(part[0], len(part))],
            sems.at[i],
        )
        for i, part in enumerate(parts)
    ]
    for copy in copies:
        copy.start()
    if start == OTHER:
        scales, start = scales_at([their_ref], offset), 0
    else:
        scales = scales_in_order([mine_ref, their_ref], offset)
    for copy, part in zip(copies, parts):
        copy.wait()
        divide_rows(rows_ref, out_ref, scales, part, start)


def divided(piece, x, mine, theirs):
    count = piece[2]
    return pl.pallas_call(
        functools.partial(divide_kernel, piece),
        in_specs=[ANY, VMEM, VMEM],
        out_specs=VMEM,
        out_shape=bf16(count, 64, 128),
        scratch_shapes=[pltpu.VMEM((count, 64, 128), jnp.float32), pltpu.SemaphoreType.DMA((pl.cdiv(count, 4),))],
        compiler_params=pltpu.CompilerParams(vmem_limit_bytes=WIDE),
        cost_estimate=cost(count * 64 * 128, 6),
        name="divide",
    )(x, mine, theirs)


def finish_kernel(pieces, *refs):
    n = len(pieces)
    rows, (mine_ref, their_ref), outs, (scale_ref, turned_ref) = refs[:n], refs[n : n + 2], refs[n + 2 : -2], refs[-2:]
    scales = scales_in_order([mine_ref, their_ref], (0, 0))
    for i, (_, start, count) in enumerate(pieces):
        divide_rows(rows[i], outs[i], scales, range(count), start)
    tile = jnp.concatenate(scales, axis=1)
    turned_ref[...] = jnp.concatenate([tile, jnp.zeros((120, 128), jnp.float32)], axis=0).T
    lane = lax.broadcasted_iota(jnp.int32, (16, 128), 1)
    out = turned_ref[pl.ds(0, 16, stride=8), :]
    for r in range(1, 8):
        part = pltpu.roll(turned_ref[pl.ds(r, 16, stride=8), :], r * 8, axis=1)
        out = jnp.where(lane >= r * 8, part, out)
    scale_ref[...] = out[:, 0:64]


def finished(pieces, rows, mine, theirs):
    n = len(pieces)
    return pl.pallas_call(
        functools.partial(finish_kernel, pieces),
        in_specs=[VMEM] * (n + 2),
        out_specs=[VMEM] * (n + 1),
        out_shape=[bf16(piece[2], 64, 128) for piece in pieces] + [f32(16, 64)],
        scratch_shapes=[pltpu.VMEM((128, 128), jnp.float32)],
        compiler_params=pltpu.CompilerParams(vmem_limit_bytes=LIMIT),
        cost_estimate=cost(sum(piece[2] for piece in pieces) * 64 * 128, 6),
        name="finish",
    )(*rows, mine, theirs)


def place_kernel(pieces, held, routed, *refs):
    n = len(pieces)
    blocks, refs = refs[:n], refs[n + held :]
    out_ref, sems = refs[routed], refs[-1]
    copies = []
    for i, (offset, start, count) in enumerate(pieces):
        z, c = sender(offset)
        column = pl.multiple_of((z * 2 + c) * 128, 128)
        target = out_ref.at[pl.ds(expert_of(start, c), count), :, pl.ds(column, 128)]
        copies.append(pltpu.make_async_copy(blocks[i], target, sems.at[i]))
    if routed:
        copies.append(pltpu.make_async_copy(refs[0], refs[2], sems.at[n]))
    for copy in copies:
        copy.start()
    for copy in copies:
        copy.wait()


def placed(pieces, blocks, shape, into=None, router=None):
    n, held, routed = len(pieces), int(into is not None), int(router is not None)
    return pl.pallas_call(
        functools.partial(place_kernel, tuple(pieces), held, routed),
        in_specs=[VMEM] * n + [ANY] * held + [VMEM] * routed,
        out_specs=[ANY] * (1 + routed),
        out_shape=[bf16(*shape)] + ([bf16(*router.shape)] if routed else []),
        scratch_shapes=[pltpu.SemaphoreType.DMA((n + routed,))],
        input_output_aliases={n: 0} if held else {},
        compiler_params=pltpu.CompilerParams(vmem_limit_bytes=LIMIT),
        cost_estimate=cost(sum(piece[2] for piece in pieces) * 64 * 128, 4),
        name="place",
    )(*blocks, *([into] if held else []), *([router] if routed else []))


def sent(piece, offset):
    pairs = [(z * 2 + c, (z + way(c) * offset[0]) % 8 * 2 + (c + offset[1]) % 2) for z in range(8) for c in range(2)]
    return lax.ppermute(piece, ZERO, pairs)


def swapped(value):
    return sent(value, (0, 1))


def per_device(train_down, router_weight, router_gain):
    experts = train_down.shape[0]
    rows = picked(RAW[:EARLY], train_down)
    keep, give, *more = local_maxima(train_down, RAW[EARLY:])
    raw = []
    for i, part in enumerate([*rows, *more]):
        raw.append(sent(part, RAW[i][0]))
    given = swapped(give)
    payload = chip_maxima(keep, given, router_weight.T, router_gain[None, :])
    shared = lax.all_to_all(payload, "zero_0", 0, 0, tiled=True)
    waiting = picked(PIECES[:READY], train_down)
    mine, lines = joined(shared)
    theirs = swapped(mine)

    kept = ((0, 0), 0, experts)
    blocks = []
    for i, piece in enumerate(PIECES):
        part = ready(piece, waiting[i], mine) if i < READY else divided(piece, train_down, mine, theirs)
        blocks.append(sent(part, piece[0]))

    lines = routed(lines, swapped(lines))
    lines, _ = lax.optimization_barrier((lines, blocks[2]))
    router = lax.all_gather(lines, "bank", axis=0, tiled=True)

    early = [divided(kept, train_down, mine, theirs)]
    *more, scale_down = finished(RAW, raw, mine, theirs)
    pieces, blocks = (kept,) + RAW + PIECES, [*early, *more, *blocks]
    shape = (experts, 64, 2048)
    ready_down, first = None, 0
    for i, n in enumerate(GROUPS):
        group = slice(first, first + n)
        out = placed(pieces[group], blocks[group], shape, ready_down, router if i == 1 else None)
        ready_down, first = out[0], first + n
        if i == 1:
            serve_router = out[1].T

    return (ready_down, scale_down, serve_router)


def solution(mesh):
    torus = Mesh(
        mesh.devices.reshape(mesh.shape["unit"], mesh.shape["bank"], 8, 2),
        ("unit", "bank", "zero_0", "zero_1"),
    )
    placed_at = (P(("unit", "bank"), None, ZERO), P(UNIT_ZERO, "bank"), P(UNIT_ZERO))
    return jax.shard_map(
        per_device,
        mesh=torus,
        in_specs=placed_at,
        out_specs=(P(("unit", "bank"), ZERO, None), P(("unit", "bank"), ZERO), P("unit", None)),
        check_vma=False,
    )
```

```python
import functools

import jax
import jax.numpy as jnp
from jax import lax
from jax.experimental import pallas as pl
from jax.experimental.pallas import tpu as pltpu
from jax.sharding import Mesh
from jax.sharding import PartitionSpec as P


ZERO = ("zero_0", "zero_1")
UNIT_ZERO = ("unit", "zero_0", "zero_1")

OWN, OTHER = -1, -2
RAW = (((4, 0), 0, 8), ((2, 0), 0, 8))
EARLY = 1
PIECES = (
    ((3, 0), OWN, 8),
    ((-3, 0), OWN, 8),
    ((4, 0), 8, 8),
    ((3, 1), 0, 16),
    ((-3, 1), 0, 16),
    ((1, 0), 0, 16),
    ((-1, 0), 0, 16),
    ((-2, 0), 0, 16),
    ((4, 1), 0, 16),
    ((3, 0), OTHER, 8),
    ((-3, 0), OTHER, 8),
    ((0, 1), 0, 16),
    ((2, 0), 8, 8),
    ((1, 1), 0, 16),
    ((-1, 1), 0, 16),
    ((2, 1), 0, 16),
    ((-2, 1), 0, 16),
)
READY = 2
GROUPS = (9, 6, 3, 2)
CARRY = tuple(next(p for p in RAW[EARLY:] + PIECES if p[0] == (z, 0)) for z in (1, 2, 3, 4, -3, -2, -1))
VMEM = pl.BlockSpec(memory_space=pltpu.VMEM)
ANY = pl.BlockSpec(memory_space=pl.ANY)
LIMIT = 4 * 1024 * 1024
WIDE = 50 * 1024 * 1024
HALF = (8, 8, 128)


def f32(*shape):
    return jax.ShapeDtypeStruct(shape, jnp.float32)


def bf16(*shape):
    return jax.ShapeDtypeStruct(shape, jnp.bfloat16)


def cost(elements, bytes_each):
    return pl.CostEstimate(flops=elements * 8, bytes_accessed=elements * bytes_each, transcendentals=0)


def way(core):
    return 1 - 2 * core


def there(offset):
    z, c = lax.axis_index("zero_0"), lax.axis_index("zero_1")
    return lax.rem(z + way(c) * offset[0] + 8, 8), lax.rem(c + offset[1], 2)


def sender(offset):
    c = lax.rem(lax.axis_index("zero_1") + offset[1], 2)
    return lax.rem(lax.axis_index("zero_0") - way(c) * offset[0] + 8, 8), c


def expert_of(start, core):
    return start if start >= 0 else core * 8 if start == OWN else (1 - core) * 8


def rows_of(piece):
    return (piece[2] * 64 + 16, 128) if piece in CARRY else (piece[2], 64, 128)


def expert_rows(ref, piece, e, first=0, count=64):
    return ref.at[pl.ds(e * 64 + first, count)] if piece in CARRY else ref.at[e, pl.ds(first, count)]


def tail_of(piece):
    return pl.ds(piece[2] * 64, 16)


def copies_of(piece):
    return piece[2] if piece in CARRY else 1


def pick(piece, x_ref, out_ref, sems, at):
    offset, start, count = piece
    z, c = there(offset)
    rows = pl.ds(pl.multiple_of((z * 2 + c) * 64, 64), 64)
    expert = expert_of(start, lax.axis_index("zero_1"))
    if piece not in CARRY:
        return [pltpu.make_async_copy(x_ref.at[pl.ds(expert, count), rows, :], out_ref, sems.at[at])]
    return [
        pltpu.make_async_copy(x_ref.at[expert + e, rows, :], expert_rows(out_ref, piece, e), sems.at[at + e])
        for e in range(count)
    ]


def picks(pieces, x_ref, refs, sems):
    copies = []
    for piece, ref in zip(pieces, refs):
        copies += pick(piece, x_ref, ref, sems, len(copies))
    return copies


def pick_kernel(pieces, x_ref, *refs):
    routed = any(piece in CARRY for piece in pieces)
    given, outs, rest = refs[: 2 * routed], refs[2 * routed : 2 * routed + len(pieces)], refs[2 * routed + len(pieces) :]
    sems = rest[-1]
    copies = picks(pieces, x_ref, outs, sems)
    for source, target in zip(given, rest):
        copies.append(pltpu.make_async_copy(source, target, sems.at[len(copies)]))
    for copy in copies:
        copy.start()
    for copy in copies:
        copy.wait()
    for piece, ref in zip(pieces, outs):
        if piece in CARRY:
            ref[tail_of(piece), :] = rest[0][...] * rest[1][...]


def picked(pieces, x, weight, gain):
    more = [weight, gain] if any(piece in CARRY for piece in pieces) else []
    return pl.pallas_call(
        functools.partial(pick_kernel, pieces),
        in_specs=[ANY] * (1 + len(more)),
        out_specs=[VMEM] * len(pieces),
        out_shape=[f32(*rows_of(piece)) for piece in pieces],
        scratch_shapes=[pltpu.VMEM(each.shape, jnp.float32) for each in more]
        + [pltpu.SemaphoreType.DMA((sum(copies_of(piece) for piece in pieces) + len(more),))],
        compiler_params=pltpu.CompilerParams(vmem_limit_bytes=WIDE),
        cost_estimate=cost(sum(piece[2] for piece in pieces) * 64 * 128, 8),
        name="pick",
    )(x, *more)


def maxima_kernel(pieces, x_ref, weight_ref, gain_ref, keep_ref, give_ref, *refs):
    halves_ref, held_ref, sems, pick_sems = refs[len(pieces) :]
    experts = x_ref.shape[0]
    lane = lax.broadcasted_iota(jnp.int32, (8, 128), 1)

    def copy(e):
        return pltpu.make_async_copy(x_ref.at[e], held_ref.at[e], sems.at[e])

    for e in range(experts):
        copy(e).start()
    more = picks(pieces, x_ref, refs, pick_sems)
    for each in more:
        each.start()
    router = weight_ref[...] * gain_ref[...]
    for piece, ref in zip(pieces, refs):
        if piece in CARRY:
            ref[tail_of(piece), :] = router

    @pl.loop(0, experts // 4)
    def _(g):
        half, part = g // 2, lax.rem(g, 2)
        for e in range(4):
            copy(g * 4 + e).wait()
        for q in range(8):
            tile = jnp.where(part == 0, jnp.zeros((8, 128), jnp.float32), halves_ref[half, q])
            for j in range(2):
                for e in range(4):
                    for r in range(8):
                        row = (q * 2 + j) * 64 + r * 8
                        top = jnp.max(jnp.abs(held_ref[g * 4 + e, row : row + 8, :]), axis=1, keepdims=True)
                        tile = jnp.where(lane == j * 64 + (part * 4 + e) * 8 + r, top, tile)
            halves_ref[half, q] = tile

    low = lax.axis_index("zero_1") == 0
    keep_ref[...] = jnp.where(low, halves_ref[0], halves_ref[1])
    give_ref[...] = jnp.where(low, halves_ref[1], halves_ref[0])
    for each in more:
        each.wait()


def local_maxima(x, pieces, weight, gain):
    return pl.pallas_call(
        functools.partial(maxima_kernel, pieces),
        in_specs=[ANY, VMEM, VMEM],
        out_specs=[VMEM] * (2 + len(pieces)),
        out_shape=[f32(*HALF), f32(*HALF)] + [f32(*rows_of(piece)) for piece in pieces],
        scratch_shapes=[
            pltpu.VMEM((2, *HALF), jnp.float32),
            pltpu.VMEM(x.shape, jnp.float32),
            pltpu.SemaphoreType.DMA((x.shape[0],)),
            pltpu.SemaphoreType.DMA((sum(copies_of(piece) for piece in pieces),)),
        ],
        compiler_params=pltpu.CompilerParams(vmem_limit_bytes=WIDE),
        name="local_maxima",
    )(x, weight, gain)


def chip_kernel(keep_ref, got_ref, out_ref):
    both = jnp.maximum(keep_ref[...], got_ref[...])
    for q in range(8):
        out_ref[q] = both


def chip_maxima(keep, got):
    return pl.pallas_call(
        chip_kernel,
        in_specs=[VMEM] * 2,
        out_specs=VMEM,
        out_shape=f32(8, *HALF),
        compiler_params=pltpu.CompilerParams(vmem_limit_bytes=LIMIT),
        name="chip",
    )(keep, got)


def joint_kernel(shared_ref, mine_ref):
    top = shared_ref[0]
    for q in range(1, 8):
        top = jnp.maximum(top, shared_ref[q])
    mine_ref[...] = top


def joined(shared):
    return pl.pallas_call(
        joint_kernel,
        in_specs=[VMEM],
        out_specs=VMEM,
        out_shape=f32(*HALF),
        compiler_params=pltpu.CompilerParams(vmem_limit_bytes=LIMIT),
        name="joint",
    )(shared)


def lines_kernel(pieces, weight_ref, gain_ref, *refs):
    z, out_ref = lax.axis_index("zero_0"), refs[-1]
    out_ref[z] = (weight_ref[...] * gain_ref[...]).astype(jnp.bfloat16)
    for piece, ref in zip(pieces, refs):
        out_ref[sender(piece[0])[0]] = ref[tail_of(piece), :].astype(jnp.bfloat16)


def lines_of(pieces, blocks, weight, gain):
    return pl.pallas_call(
        functools.partial(lines_kernel, pieces),
        in_specs=[VMEM] * (2 + len(pieces)),
        out_specs=VMEM,
        out_shape=bf16(8, 16, 128),
        compiler_params=pltpu.CompilerParams(vmem_limit_bytes=LIMIT),
        name="lines",
    )(weight, gain, *blocks)


def route_kernel(mine_ref, their_ref, out_ref):
    low = lax.axis_index("zero_1") == 0
    for q in range(8):
        mine, theirs = mine_ref[q], their_ref[q]
        out_ref[:, q * 256 : q * 256 + 128] = jnp.where(low, mine, theirs)
        out_ref[:, q * 256 + 128 : q * 256 + 256] = jnp.where(low, theirs, mine)


def routed(mine, theirs):
    return pl.pallas_call(
        route_kernel,
        in_specs=[VMEM] * 2,
        out_specs=VMEM,
        out_shape=bf16(16, 2048),
        compiler_params=pltpu.CompilerParams(vmem_limit_bytes=LIMIT),
        name="route",
    )(mine, theirs)


def scales_at(refs, offset):
    z, c = there(offset)
    tiles = [ref[z] for ref in refs]
    return [jnp.where(c == 0, tile[:, 0:64], tile[:, 64:128]) for tile in tiles]


def scales_in_order(refs, offset):
    own, other = scales_at(refs, offset)
    low = lax.axis_index("zero_1") == 0
    return [jnp.where(low, own, other), jnp.where(low, other, own)]


def divide_rows(rows, write, scales, experts, start):
    for e in experts:
        scale = scales[(start + e) // 8]
        for r in range(0, 8, 2):
            lane = (start + e) % 8 * 8 + r
            both = jnp.concatenate([scale[:, lane : lane + 1], scale[:, lane + 1 : lane + 2]], axis=0)
            write(e, r, (rows(e, r) / both).astype(jnp.bfloat16))


def reads(piece, ref):
    return lambda e, r: expert_rows(ref, piece, e, r * 8, 16)[...]


def writes(piece, ref):
    def write(e, r, value):
        expert_rows(ref, piece, e, r * 8, 16)[...] = value

    return write


def ready_kernel(piece, rows_ref, mine_ref, out_ref):
    scales = scales_at([mine_ref], piece[0])
    divide_rows(reads(piece, rows_ref), writes(piece, out_ref), scales, range(8), 0)
    if piece in CARRY:
        out_ref[tail_of(piece), :] = rows_ref[tail_of(piece), :].astype(jnp.bfloat16)


def ready(piece, rows, mine):
    return pl.pallas_call(
        functools.partial(ready_kernel, piece),
        in_specs=[VMEM, VMEM],
        out_specs=VMEM,
        out_shape=bf16(*rows_of(piece)),
        compiler_params=pltpu.CompilerParams(vmem_limit_bytes=LIMIT),
        cost_estimate=cost(8 * 64 * 128, 6),
        name="ready",
    )(rows, mine)


def divide_kernel(piece, x_ref, mine_ref, their_ref, *refs):
    out_ref, rows_ref, sems = refs[-3:]
    offset, start, count = piece
    z, c = there(offset)
    first = pl.multiple_of((z * 2 + c) * 64, 64)
    expert = expert_of(start, lax.axis_index("zero_1"))
    parts = [range(e, min(e + 4, count)) for e in range(0, count, 4)]
    copies = [
        pltpu.make_async_copy(
            x_ref.at[pl.ds(expert + part[0], len(part)), pl.ds(first, 64), :],
            rows_ref.at[pl.ds(part[0], len(part))],
            sems.at[i],
        )
        for i, part in enumerate(parts)
    ]
    for copy in copies:
        copy.start()
    if start == OTHER:
        scales, start = scales_at([their_ref], offset), 0
    else:
        scales = scales_in_order([mine_ref, their_ref], offset)
    if piece in CARRY:
        out_ref[tail_of(piece), :] = (refs[0][...] * refs[1][...]).astype(jnp.bfloat16)
    for copy, part in zip(copies, parts):
        copy.wait()
        divide_rows(lambda e, r: rows_ref[e, r * 8 : r * 8 + 16, :], writes(piece, out_ref), scales, part, start)


def divided(piece, x, mine, theirs, weight, gain):
    count = piece[2]
    more = [weight, gain] if piece in CARRY else []
    return pl.pallas_call(
        functools.partial(divide_kernel, piece),
        in_specs=[ANY] + [VMEM] * (2 + len(more)),
        out_specs=VMEM,
        out_shape=bf16(*rows_of(piece)),
        scratch_shapes=[pltpu.VMEM((count, 64, 128), jnp.float32), pltpu.SemaphoreType.DMA((pl.cdiv(count, 4),))],
        compiler_params=pltpu.CompilerParams(vmem_limit_bytes=WIDE),
        cost_estimate=cost(count * 64 * 128, 6),
        name="divide",
    )(x, mine, theirs, *more)


def finish_kernel(pieces, *refs):
    n = len(pieces)
    rows, (mine_ref, their_ref), outs, (scale_ref, turned_ref) = refs[:n], refs[n : n + 2], refs[n + 2 : -2], refs[-2:]
    scales = scales_in_order([mine_ref, their_ref], (0, 0))
    for i, piece in enumerate(pieces):
        plain = writes(((0, 0), 0, 0), outs[i])
        divide_rows(reads(piece, rows[i]), plain, scales, range(piece[2]), piece[1])
    tile = jnp.concatenate(scales, axis=1)
    turned_ref[...] = jnp.concatenate([tile, jnp.zeros((120, 128), jnp.float32)], axis=0).T
    lane = lax.broadcasted_iota(jnp.int32, (16, 128), 1)
    out = turned_ref[pl.ds(0, 16, stride=8), :]
    for r in range(1, 8):
        part = pltpu.roll(turned_ref[pl.ds(r, 16, stride=8), :], r * 8, axis=1)
        out = jnp.where(lane >= r * 8, part, out)
    scale_ref[...] = out[:, 0:64]


def finished(pieces, rows, mine, theirs):
    n = len(pieces)
    return pl.pallas_call(
        functools.partial(finish_kernel, pieces),
        in_specs=[VMEM] * (n + 2),
        out_specs=[VMEM] * (n + 1),
        out_shape=[bf16(piece[2], 64, 128) for piece in pieces] + [f32(16, 64)],
        scratch_shapes=[pltpu.VMEM((128, 128), jnp.float32)],
        compiler_params=pltpu.CompilerParams(vmem_limit_bytes=LIMIT),
        cost_estimate=cost(sum(piece[2] for piece in pieces) * 64 * 128, 6),
        name="finish",
    )(*rows, mine, theirs)


def place_kernel(pieces, held, routed, *refs):
    n = len(pieces)
    blocks, refs = refs[:n], refs[n + held :]
    out_ref, sems = refs[routed], refs[-1]
    copies = []
    for i, (offset, start, count) in enumerate(pieces):
        z, c = sender(offset)
        column = pl.multiple_of((z * 2 + c) * 128, 128)
        expert, columns = expert_of(start, c), pl.ds(column, 128)
        if len(blocks[i].shape) == 3:
            moves = [(blocks[i], out_ref.at[pl.ds(expert, count), :, columns])]
        else:
            moves = [(blocks[i].at[pl.ds(e * 64, 64)], out_ref.at[expert + e, :, columns]) for e in range(count)]
        for source, target in moves:
            copies.append(pltpu.make_async_copy(source, target, sems.at[len(copies)]))
    if routed:
        copies.append(pltpu.make_async_copy(refs[0], refs[2], sems.at[len(copies)]))
    for copy in copies:
        copy.start()
    for copy in copies:
        copy.wait()


def placed(pieces, blocks, shape, into=None, router=None):
    n, held, routed = len(pieces), int(into is not None), int(router is not None)
    return pl.pallas_call(
        functools.partial(place_kernel, tuple(pieces), held, routed),
        in_specs=[VMEM] * n + [ANY] * held + [VMEM] * routed,
        out_specs=[ANY] * (1 + routed),
        out_shape=[bf16(*shape)] + ([bf16(*router.shape)] if routed else []),
        scratch_shapes=[pltpu.SemaphoreType.DMA((sum(b.shape[0] // 64 if b.ndim == 2 else 1 for b in blocks) + routed,))],
        input_output_aliases={n: 0} if held else {},
        compiler_params=pltpu.CompilerParams(vmem_limit_bytes=LIMIT),
        cost_estimate=cost(sum(piece[2] for piece in pieces) * 64 * 128, 4),
        name="place",
    )(*blocks, *([into] if held else []), *([router] if routed else []))


def sent(piece, offset):
    pairs = [(z * 2 + c, (z + way(c) * offset[0]) % 8 * 2 + (c + offset[1]) % 2) for z in range(8) for c in range(2)]
    return lax.ppermute(piece, ZERO, pairs)


def swapped(value):
    return sent(value, (0, 1))


def per_device(train_down, router_weight, router_gain):
    experts = train_down.shape[0]
    router = (router_weight.T, router_gain[None, :])
    rows = picked(RAW[:EARLY], train_down, *router)
    keep, give, *more = local_maxima(train_down, RAW[EARLY:], *router)
    raw = []
    for i, part in enumerate([*rows, *more]):
        raw.append(sent(part, RAW[i][0]))
    given = swapped(give)
    payload = chip_maxima(keep, given)
    shared = lax.all_to_all(payload, "zero_0", 0, 0, tiled=True)
    waiting = picked(PIECES[:READY], train_down, *router)
    mine = joined(shared)
    theirs = swapped(mine)

    kept = ((0, 0), 0, experts)
    blocks = []
    for i, piece in enumerate(PIECES):
        part = ready(piece, waiting[i], mine) if i < READY else divided(piece, train_down, mine, theirs, *router)
        blocks.append(sent(part, piece[0]))

    every = dict(zip(RAW + PIECES, [*raw, *blocks]))
    lines = lines_of(CARRY, [every[piece] for piece in CARRY], *router)
    lines = routed(lines, swapped(lines))
    gathered = lax.all_gather(lines, "bank", axis=0, tiled=True)

    early = [divided(kept, train_down, mine, theirs, *router)]
    *more, scale_down = finished(RAW, raw, mine, theirs)
    pieces, blocks = (kept,) + RAW + PIECES, [*early, *more, *blocks]
    shape = (experts, 64, 2048)
    ready_down, first = None, 0
    for i, n in enumerate(GROUPS):
        group = slice(first, first + n)
        out = placed(pieces[group], blocks[group], shape, ready_down, gathered if i == 1 else None)
        ready_down, first = out[0], first + n
        if i == 1:
            serve_router = out[1].T

    return (ready_down, scale_down, serve_router)


def solution(mesh):
    torus = Mesh(
        mesh.devices.reshape(mesh.shape["unit"], mesh.shape["bank"], 8, 2),
        ("unit", "bank", "zero_0", "zero_1"),
    )
    placed_at = (P(("unit", "bank"), None, ZERO), P(UNIT_ZERO, "bank"), P(UNIT_ZERO))
    return jax.shard_map(
        per_device,
        mesh=torus,
        in_specs=placed_at,
        out_specs=(P(("unit", "bank"), ZERO, None), P(("unit", "bank"), ZERO), P("unit", None)),
        check_vma=False,
    )
```
